32 devices in a mesh: parts: 2 (over x), inner: 16 (over z, y, core).
Axes of the slice: x: 2, y: 2, z: 4, core: 2. Of those that a mesh axis runs over, the one named last changes fastest.
Arguments:
- stem_slab: bfloat16 [2, 16384, 1024], P(None, ('parts', 'inner')), parts along dimension 1, may hold values from -6 to 6
- branches: bfloat16 [3, 2, 1024, 1024], P(None, None, 'inner'), may hold values from -0.1875 to 0.1875
- column_order: int32 [3, 1024], replicated, may hold values from 0 to 1023, each once within a row
Outputs:
- result_slab: bfloat16 [2, 16384, 1024], P(None, ('parts', 'inner')), parts along dimension 1
The draws below stay inside these ranges and needn't reach their ends.
There are 2 independent parts, one for each index of `parts`. The reference program is written for one: setup_inputs(seed, part) draws one part's arguments, and reference() takes and returns one part's arrays. A program takes and returns all parts, laid end to end along the dimension named above; an argument that names none is the same for every part. Nothing has to cross between parts.
Inputs may be any that keep to these rules, and one draw needn't show every extreme that they name: Each row of column_order names every number from 0 to 1023 exactly once.
All inputs are finite; a program needn't handle non-finite values.
Results may differ from the reference program's by a relative error of at most 0.0057.
Values may be sent and summed in bfloat16 or wider, within the bound.
A program may use at most 64 MiB of HBM per device.

```python
import jax
import jax.numpy as jnp

BRANCH = 1024
ROWS_DEV = 512
STEPS = 3
ROWS = 8192
N_INNER = 16


def raised(array, key, source, target, blocks, factor):
    owner, partner = [(jnp.arange(array.shape[position]) // (array.shape[position] // blocks)).reshape([-1 if axis == position else 1 for axis in range(array.ndim)]) for position in (source, target)]
    chosen = jax.random.permutation(key, blocks)[partner]
    strong = (owner == chosen) | (owner == (partner + blocks // 2) % blocks)
    return jnp.where(strong, factor * array, array)


def block_scale(key, shape, pieces, least, top_value):
    loudness = 1.0
    for position, blocks in pieces:
        draws = jax.random.uniform(jax.random.fold_in(jax.random.fold_in(key, 6), position), (blocks,), jnp.float32, least / len(pieces), top_value / len(pieces))
        loudness = loudness * jnp.repeat(jnp.exp(draws), shape[position] // blocks).reshape((-1,) + (1,) * (len(shape) - 1 - position))
    return loudness


def noise(stream_key, extent, spread, limit, cuts=(), held_as=jnp.bfloat16):
    drawn = jax.random.normal(stream_key, extent, jnp.float32) * spread
    if len(cuts) > 0:
        drawn = block_scale(stream_key, extent, cuts, -0.22, 0.18) * drawn
    return jnp.clip(drawn, min=-limit, max=limit).astype(held_as)


def gaussian_with(own_key, extent, scale, most, cuts, heavy, kind=jnp.bfloat16):
    array = scale * jax.random.normal(own_key, extent, jnp.float32)
    if cuts:
        array = array * block_scale(own_key, extent, cuts, -0.22, 0.18)
    return jnp.clip(raised(array, jax.random.fold_in(own_key, 3), *heavy), -most, most).astype(kind)


def setup_inputs(seed: int = 0, part: int = 0) -> dict:
    key_list = jax.random.split(jax.random.key(seed), 4)
    own_keys = jax.random.split(jax.random.fold_in(key_list[3], part), 4)
    return {
        "stem_slab": noise(own_keys[0], (2, ROWS, BRANCH), 1.0, 6.0, ((1, 16),)),
        "branches": gaussian_with(key_list[1], (STEPS, 2, BRANCH, BRANCH), (2 * BRANCH) ** -0.5, 0.1875, ((2, 16),), (2, 3, 16, 2.0)),
        "column_order": jax.vmap(lambda own: jax.random.permutation(own, BRANCH))(jax.random.split(key_list[2], STEPS)).reshape((STEPS, BRANCH)).astype(jnp.int32),
    }


def contract(slab, order_row, pair):
    picked = jnp.take(slab, order_row.astype(jnp.int32), axis=2)
    real_part = jnp.dot(picked[0], pair[0], preferred_element_type=jnp.float32) - jnp.dot(picked[1], pair[1], preferred_element_type=jnp.float32)
    imag_part = jnp.dot(picked[0], pair[1], preferred_element_type=jnp.float32) + jnp.dot(picked[1], pair[0], preferred_element_type=jnp.float32)
    return jnp.stack([real_part, imag_part]).astype(jnp.bfloat16)


def swap_blocks(slab):
    width = BRANCH // N_INNER
    blocks = slab.reshape(2, N_INNER, ROWS_DEV, N_INNER, width)
    return jnp.transpose(blocks, (0, 3, 2, 1, 4)).reshape(2, N_INNER * ROWS_DEV, BRANCH)


def reference(stem_slab, branches, column_order):
    current = stem_slab
    for section_index in range(STEPS):
        if section_index > 0:
            current = swap_blocks(current)
        current = contract(current, column_order[section_index], branches[section_index])
    return current
```

```python
import functools

import jax
import jax.numpy as jnp
from jax import lax
from jax.experimental import pallas as pl
from jax.experimental.pallas import tpu as pltpu
from jax.sharding import PartitionSpec as P

CORES = 2
YS = 2
CHUNKS = 4
TILE = 256
LANES = 128
F32 = jnp.float32
BF16 = jnp.bfloat16
MESH_ID = pl.DeviceIdType.MESH


def add_block(ordered, block_rows):
    real_part = jnp.dot(ordered[0], block_rows[0], preferred_element_type=F32) - jnp.dot(
        ordered[1], block_rows[1], preferred_element_type=F32
    )
    imag_part = jnp.dot(ordered[0], block_rows[1], preferred_element_type=F32) + jnp.dot(
        ordered[1], block_rows[0], preferred_element_type=F32
    )
    return jnp.stack([real_part, imag_part])


def folded(slab, order_row, branch_slice):
    ordered = jnp.take(slab, order_row, axis=2)
    summed = add_block(ordered, lax.all_gather(branch_slice, "inner", axis=1, tiled=True))
    return summed.astype(BF16)


def plain(stem_slab, branches, column_order):
    current = folded(stem_slab, column_order[0], branches[0])
    for section_index in range(1, branches.shape[0]):
        current = lax.all_to_all(current, "inner", split_axis=2, concat_axis=2, tiled=True)
        current = folded(current, column_order[section_index], branches[section_index])
    return current


def kernel(
    n, stem, branches, order, out, gathered, onehot, picked, wide, send, recv,
    own_sem, zs_sem, zr_sem, ys_sem, yr_sem, cs_sem, cr_sem, as_sem, ar_sem,
):
    sections = branches.shape[0]
    depth = branches.shape[2]
    total = n * depth
    columns = branches.shape[3]
    chunk = send.shape[3]
    plane = CORES * YS
    nz = n // plane
    me = lax.axis_index("inner")
    z = me // plane
    low = me % plane
    y = low // CORES
    core = low % CORES
    y_peer = z * plane + (1 - y) * CORES + core
    core_peer = z * plane + y * CORES + (1 - core)

    barrier = pltpu.get_barrier_semaphore()

    @pl.loop(1, n)
    def _(hop):
        pl.semaphore_signal(
            barrier, inc=1, device_id={"inner": lax.rem(me + hop, n)}, device_id_type=MESH_ID
        )

    pl.semaphore_wait(barrier, n - 1)

    def remote(src, dst, send_sem, recv_sem, device):
        return pltpu.make_async_remote_copy(
            src_ref=src, dst_ref=dst, send_sem=send_sem, recv_sem=recv_sem,
            device_id={"inner": device}, device_id_type=MESH_ID,
        )

    def slot_of(zz):
        return zz * plane + low

    def own_or(s, t, slot):
        return branches.at[s] if t == 0 else gathered.at[s, slot]

    def z_copy(s, t, way):
        zz = z - t if way == 0 else z + t
        target = me + plane if way == 0 else me - plane
        slot = slot_of(zz)
        return remote(
            own_or(s, t, slot), gathered.at[s, slot], zs_sem.at[s, t, way], zr_sem.at[s, t, way], target
        )

    def z_sends(t, way):
        return (z - t >= 0) & (z + 1 < nz) if way == 0 else (z + t < nz) & (z >= 1)

    def z_holds(t, way):
        return z - t >= 0 if way == 0 else z + t < nz

    def y_copy(s, t, zz):
        slot = slot_of(zz)
        return remote(own_or(s, t, slot), gathered.at[s, slot], ys_sem.at[s, zz], yr_sem.at[s, zz], y_peer)

    def core_copy(s, t, slot):
        return remote(own_or(s, t, slot), gathered.at[s, slot], cs_sem.at[s], cr_sem.at[s], core_peer)

    def begin(s):
        for way in (0, 1):
            @pl.when(z_sends(0, way))
            def _():
                z_copy(s, 0, way).start()
        y_copy(s, 0, z).start()
        core_copy(s, 0, me).start()
        pltpu.make_async_copy(branches.at[s], gathered.at[s, me], own_sem.at[s]).start()

    def z_step(s, t):
        for way in (0, 1):
            zz = z - t if way == 0 else z + t

            @pl.when(z_holds(t, way))
            def _():
                slot = slot_of(zz)
                remote(
                    gathered.at[s, slot], gathered.at[s, slot], zs_sem.at[s, t - 1, way],
                    zr_sem.at[s, t - 1, way], y_peer,
                ).wait_recv()

                if t < nz - 1:
                    @pl.when(z_sends(t, way))
                    def _():
                        z_copy(s, t, way).start()

                y_copy(s, t, zz).start()
                core_copy(s, t, slot).start()

    def y_step(s, t):
        ways = (0,) if t == 0 else (0, 1)
        for way in ways:
            zz = z - t if way == 0 else z + t

            @pl.when(z_holds(t, way))
            def _():
                slot = zz * plane + (1 - y) * CORES + core
                remote(
                    gathered.at[s, slot], gathered.at[s, slot], ys_sem.at[s, zz], yr_sem.at[s, zz], y_peer
                ).wait_recv()
                core_copy(s, 1, slot).start()

    def finish(s):
        half = gathered.at[s, pl.ds(0, n // CORES)]
        remote(half, half, cs_sem.at[s], cr_sem.at[s], core_peer).wait_recv()
        pltpu.make_async_copy(branches.at[s], gathered.at[s, me], own_sem.at[s]).wait()

    def build_onehot(s):
        @pl.loop(0, total // LANES)
        def _(i):
            rows = pl.ds(pl.multiple_of(i * LANES, LANES), LANES)
            target = lax.broadcasted_iota(jnp.int32, (LANES, total), 0) + i * LANES
            onehot[rows, :] = jnp.where(order[s : s + 1, :] == target, 1.0, 0.0).astype(BF16)

    def pick_stem():
        @pl.loop(0, total // TILE)
        def _(j):
            cols = pl.ds(pl.multiple_of(j * TILE, TILE), TILE)
            for p in range(2):
                picked[p, :, cols] = jnp.dot(
                    stem[p], onehot[:, cols], preferred_element_type=F32
                ).astype(BF16)

    def prepare(s):
        build_onehot(s)
        groups = TILE // depth

        @pl.loop(0, columns // TILE)
        def _(j):
            cols = pl.ds(pl.multiple_of(j * TILE, TILE), TILE)
            real_rows = gathered[s, :, 0, :, cols].reshape(total, TILE)
            imag_rows = gathered[s, :, 1, :, cols].reshape(total, TILE)
            for i in range(total // TILE):
                rows = onehot[i * TILE : (i + 1) * TILE, :]
                real = jnp.dot(rows, real_rows, preferred_element_type=F32)
                imag = jnp.dot(rows, imag_rows, preferred_element_type=F32)
                real_b = real.astype(BF16)
                imag_b = imag.astype(BF16)
                minus_b = (-imag).astype(BF16)
                for b in range(groups):
                    part = slice(b * depth, (b + 1) * depth)
                    at = (i * groups + b) * 2 * depth
                    wide[s - 1, 0, at : at + depth, cols] = real_b[part]
                    wide[s - 1, 0, at + depth : at + 2 * depth, cols] = minus_b[part]
                    wide[s - 1, 1, at : at + depth, cols] = imag_b[part]
                    wide[s - 1, 1, at + depth : at + 2 * depth, cols] = real_b[part]

    low_half = lax.broadcasted_iota(jnp.int32, (chunk, LANES), 1) < LANES // 2

    def pack(step, k, j, real, imag):
        for t in range(TILE // LANES):
            re = real[:, t * LANES : (t + 1) * LANES]
            im = imag[:, t * LANES : (t + 1) * LANES]
            first = jnp.where(low_half, re, pltpu.roll(im, LANES // 2, 1))
            second = jnp.where(low_half, pltpu.roll(re, LANES // 2, 1), im)
            base = (j * (TILE // LANES) + t) * 2
            send[step, k, base] = first.astype(BF16)
            send[step, k, base + 1] = second.astype(BF16)

    def swap_start(step, k):
        recv[step, k, me] = send[step, k, me]

        @pl.loop(1, n)
        def _(hop):
            target = lax.rem(me + hop, n)
            remote(
                send.at[step, k, target], recv.at[step, k, me], as_sem.at[step, k], ar_sem.at[step, k], target
            ).start()

    def swap_wait(step, k):
        part = pl.ds(0, n - 1)
        return remote(
            send.at[step, k, part], recv.at[step, k, part], as_sem.at[step, k], ar_sem.at[step, k], core_peer
        )

    def first_section(k):
        rows = slice(k * chunk, (k + 1) * chunk)

        @pl.loop(0, columns // TILE)
        def _(j):
            cols = pl.ds(pl.multiple_of(j * TILE, TILE), TILE)
            real_rows = gathered[0, :, 0, :, cols].reshape(total, TILE)
            imag_rows = gathered[0, :, 1, :, cols].reshape(total, TILE)
            a, b = picked[0, rows, :], picked[1, rows, :]
            dot = functools.partial(jnp.dot, preferred_element_type=F32)
            pack(0, k, j, dot(a, real_rows) - dot(b, imag_rows), dot(a, imag_rows) + dot(b, real_rows))

    def later_section(s, k):
        rows = slice(k * chunk, (k + 1) * chunk)

        @pl.loop(0, columns // TILE)
        def _(j):
            cols = pl.ds(pl.multiple_of(j * TILE, TILE), TILE)
            left = jnp.concatenate([recv[s - 1, k, g] for g in range(n)], axis=1)
            real = jnp.dot(left, wide[s - 1, 0, :, cols], preferred_element_type=F32)
            imag = jnp.dot(left, wide[s - 1, 1, :, cols], preferred_element_type=F32)
            if s < sections - 1:
                pack(s, k, j, real, imag)
            else:
                out[0, rows, cols] = real.astype(BF16)
                out[1, rows, cols] = imag.astype(BF16)

    begin(0)
    build_onehot(0)
    pick_stem()
    z_step(0, 1)
    y_step(0, 0)
    begin(1)
    for t in range(2, nz):
        z_step(0, t)
        y_step(0, t - 1)
        z_step(1, t - 1)
    begin(2)
    y_step(0, nz - 1)
    finish(0)
    for k in range(CHUNKS):
        first_section(k)
        swap_start(0, k)
    z_step(1, nz - 1)
    for t in range(nz):
        y_step(1, t)
    for t in range(1, nz):
        z_step(2, t)
    finish(1)
    prepare(1)
    for k in range(CHUNKS):
        swap_wait(0, k).wait_recv()
        later_section(1, k)
        swap_start(1, k)
        if k == CHUNKS // 2:
            for t in range(nz):
                y_step(2, t)
            finish(2)
            prepare(2)
    for k in range(CHUNKS):
        swap_wait(1, k).wait_recv()
        later_section(2, k)

    for step in range(sections - 1):
        for k in range(CHUNKS):
            swap_wait(step, k).wait_send()
    for s in range(sections):
        for t in range(nz - 1):
            for way in (0, 1):
                @pl.when(z_sends(t, way))
                def _():
                    z_copy(s, t, way).wait_send()
        for zz in range(nz):
            y_copy(s, 1, zz).wait_send()
        half = gathered.at[s, pl.ds(0, n // CORES)]
        remote(half, half, cs_sem.at[s], cr_sem.at[s], core_peer).wait_send()


def fused(n, stem_slab, branches, column_order):
    sections, _, depth, columns = branches.shape
    rows = stem_slab.shape[1]
    chunk = rows // CHUNKS
    nz = n // (CORES * YS)
    total = n * depth
    dma = pltpu.SemaphoreType.DMA
    return pl.pallas_call(
        functools.partial(kernel, n),
        out_shape=jax.ShapeDtypeStruct(stem_slab.shape, BF16),
        in_specs=[pl.BlockSpec(memory_space=pltpu.VMEM)] * 3,
        out_specs=pl.BlockSpec(memory_space=pltpu.VMEM),
        scratch_shapes=[
            pltpu.VMEM((sections, n, 2, depth, columns), BF16),
            pltpu.VMEM((total, total), BF16),
            pltpu.VMEM(stem_slab.shape, BF16),
            pltpu.VMEM((sections - 1, 2, 2 * total, columns), BF16),
            pltpu.VMEM((sections - 1, CHUNKS, n, chunk, LANES), BF16),
            pltpu.VMEM((sections - 1, CHUNKS, n, chunk, LANES), BF16),
            dma((sections,)),
            dma((sections, nz, 2)),
            dma((sections, nz, 2)),
            dma((sections, nz)),
            dma((sections, nz)),
            dma((sections,)),
            dma((sections,)),
            dma((sections - 1, CHUNKS)),
            dma((sections - 1, CHUNKS)),
        ],
        compiler_params=pltpu.CompilerParams(
            collective_id=0, has_side_effects=True, vmem_limit_bytes=60 * 2**20
        ),
    )(stem_slab, branches, column_order)


def solution(mesh):
    n = mesh.shape["inner"]

    def local(stem_slab, branches, column_order):
        columns = branches.shape[3]
        fits = 2 * (columns // n) == LANES and n % (CORES * YS) == 0 and n > CORES * YS
        if fits and branches.shape[0] == 3 and columns == n * branches.shape[2]:
            return fused(n, stem_slab, branches, column_order)
        return plain(stem_slab, branches, column_order)

    in_specs = (P(None, ("parts", "inner"), None), P(None, None, "inner", None), P())
    out_specs = P(None, ("parts", "inner"), None)
    return jax.shard_map(local, mesh=mesh, in_specs=in_specs, out_specs=out_specs, check_vma=False)
```

```python
import functools

import jax
import jax.numpy as jnp
from jax import lax
from jax.experimental import pallas as pl
from jax.experimental.pallas import tpu as pltpu
from jax.sharding import PartitionSpec as P

CORES = 2
YS = 2
CHUNKS = 4
TILE = 256
LANES = 128
F32 = jnp.float32
BF16 = jnp.bfloat16
MESH_ID = pl.DeviceIdType.MESH


def add_block(ordered, block_rows):
    real_part = jnp.dot(ordered[0], block_rows[0], preferred_element_type=F32) - jnp.dot(
        ordered[1], block_rows[1], preferred_element_type=F32
    )
    imag_part = jnp.dot(ordered[0], block_rows[1], preferred_element_type=F32) + jnp.dot(
        ordered[1], block_rows[0], preferred_element_type=F32
    )
    return jnp.stack([real_part, imag_part])


def folded(slab, order_row, branch_slice):
    ordered = jnp.take(slab, order_row, axis=2)
    summed = add_block(ordered, lax.all_gather(branch_slice, "inner", axis=1, tiled=True))
    return summed.astype(BF16)


def plain(stem_slab, branches, column_order):
    current = folded(stem_slab, column_order[0], branches[0])
    for section_index in range(1, branches.shape[0]):
        current = lax.all_to_all(current, "inner", split_axis=2, concat_axis=2, tiled=True)
        current = folded(current, column_order[section_index], branches[section_index])
    return current


def kernel(
    n, stem_hbm, branches, order, out_hbm, stem, out, gathered, onehot, picked, wide, send, recv,
    own_sem, zs_sem, zr_sem, xs_sem, xr_sem, ys_sem, yr_sem, ds_sem, dr_sem, cs_sem, cr_sem, as_sem, ar_sem,
    in_sem, out_sem,
):
    sections = branches.shape[0]
    depth = branches.shape[2]
    total = n * depth
    columns = branches.shape[3]
    chunk = send.shape[3]
    plane = CORES * YS
    nz = n // plane
    me = lax.axis_index("inner")
    x = lax.axis_index("parts")
    z = me // plane
    low = me % plane
    y = low // CORES
    core = low % CORES
    other_low = (1 - y) * CORES + core
    x_peer = {"parts": 1 - x}
    y_peer = {"inner": z * plane + other_low}
    core_peer = {"inner": z * plane + y * CORES + (1 - core)}

    stem_copy = pltpu.make_async_copy(stem_hbm, stem, in_sem)
    stem_copy.start()

    barrier = pltpu.get_barrier_semaphore()

    @pl.loop(1, n)
    def _(hop):
        pl.semaphore_signal(
            barrier, inc=1, device_id={"inner": lax.rem(me + hop, n)}, device_id_type=MESH_ID
        )

    pl.semaphore_signal(barrier, inc=1, device_id=x_peer, device_id_type=MESH_ID)
    pl.semaphore_wait(barrier, n)

    def remote(src, dst, send_sem, recv_sem, device):
        return pltpu.make_async_remote_copy(
            src_ref=src, dst_ref=dst, send_sem=send_sem, recv_sem=recv_sem,
            device_id=device, device_id_type=MESH_ID,
        )

    def block(s, zz, across, p, own=False):
        slot = zz * plane + (other_low if across else low)
        return (branches.at[s, p] if own else gathered.at[s, slot, p]), gathered.at[s, slot, p]

    def z_of(t, way):
        return z - t if way == 0 else z + t

    def z_copy(s, t, way):
        src, dst = block(s, z_of(t, way), False, x, own=t == 0)
        target = {"inner": me + plane if way == 0 else me - plane}
        return remote(src, dst, zs_sem.at[s, t, way], zr_sem.at[s, t, way], target)

    def z_sends(t, way):
        return (z - t >= 0) & (z + 1 < nz) if way == 0 else (z + t < nz) & (z >= 1)

    def z_holds(t, way):
        return z - t >= 0 if way == 0 else z + t < nz

    def x_copy(s, zz):
        src, dst = block(s, zz, False, x)
        return remote(src, dst, xs_sem.at[s, zz], xr_sem.at[s, zz], x_peer)

    def y_copy(s, zz, own=False):
        src, dst = block(s, zz, False, x, own)
        return remote(src, dst, ys_sem.at[s, zz], yr_sem.at[s, zz], y_peer)

    def diagonal_x(s, zz):
        src, dst = block(s, zz, True, x)
        return remote(src, dst, ds_sem.at[s, zz], dr_sem.at[s, zz], x_peer)

    def diagonal_y(s, zz, own=False):
        src, dst = block(s, zz, False, 1 - x, own)
        return remote(src, dst, ds_sem.at[s, zz], dr_sem.at[s, zz], y_peer)

    def core_send(s, zz, across, p, own=False):
        src, dst = block(s, zz, across, p, own)
        remote(src, dst, cs_sem.at[s], cr_sem.at[s], core_peer).start()

    def arrived(s, zz, across, p, sem):
        _, dst = block(s, zz, across, p)
        remote(dst, dst, cs_sem.at[s], sem, core_peer).wait_recv()

    def begin_z(s):
        for way in (0, 1):
            @pl.when(z_sends(0, way))
            def _():
                z_copy(s, 0, way).start()

    def begin_side(s):
        y_copy(s, z, own=True).start()

        @pl.when(core == 1)
        def _():
            diagonal_y(s, z, own=True).start()

        core_send(s, z, False, x, own=True)
        core_send(s, z, False, 1 - x, own=True)
        pltpu.make_async_copy(branches.at[s], gathered.at[s, me], own_sem.at[s]).start()

    def z_step(s, t):
        for way in (0, 1):
            @pl.when(z_holds(t, way))
            def _():
                arrived(s, z_of(t, way), False, x, zr_sem.at[s, t - 1, way])

                if t < nz - 1:
                    @pl.when(z_sends(t, way))
                    def _():
                        z_copy(s, t, way).start()

    def side_send(s, t):
        for way in (0, 1):
            @pl.when(z_holds(t, way))
            def _():
                zz = z_of(t, way)
                x_copy(s, zz).start()
                y_copy(s, zz).start()
                core_send(s, zz, False, x)

    def side_step(s, t):
        for way in (0,) if t == 0 else (0, 1):
            @pl.when(z_holds(t, way))
            def _():
                zz = z_of(t, way)
                arrived(s, zz, True, x, yr_sem.at[s, zz])

                @pl.when(core == 0)
                def _():
                    diagonal_x(s, zz).start()

                core_send(s, zz, True, x)
                if t > 0:
                    arrived(s, zz, False, 1 - x, xr_sem.at[s, zz])

                    @pl.when(core == 1)
                    def _():
                        diagonal_y(s, zz).start()

                    core_send(s, zz, False, 1 - x)

    def diagonal_step(s, t):
        for way in (0,) if t == 0 else (0, 1):
            @pl.when(z_holds(t, way))
            def _():
                zz = z_of(t, way)
                arrived(s, zz, True, 1 - x, dr_sem.at[s, zz])
                core_send(s, zz, True, 1 - x)

    def finish(s):
        half = gathered.at[s, pl.ds(0, n // CORES)]
        remote(half, half, cs_sem.at[s], cr_sem.at[s], core_peer).wait_recv()
        pltpu.make_async_copy(branches.at[s], gathered.at[s, me], own_sem.at[s]).wait()

    def build_onehot(s):
        @pl.loop(0, total // LANES)
        def _(i):
            rows = pl.ds(pl.multiple_of(i * LANES, LANES), LANES)
            target = lax.broadcasted_iota(jnp.int32, (LANES, total), 0) + i * LANES
            onehot[rows, :] = jnp.where(order[s : s + 1, :] == target, 1.0, 0.0).astype(BF16)

    def pick_stem():
        @pl.loop(0, total // TILE)
        def _(j):
            cols = pl.ds(pl.multiple_of(j * TILE, TILE), TILE)
            for p in range(2):
                picked[p, :, cols] = jnp.dot(
                    stem[p], onehot[:, cols], preferred_element_type=F32
                ).astype(BF16)

    def prepare(s):
        build_onehot(s)
        groups = TILE // depth

        @pl.loop(0, columns // TILE)
        def _(j):
            cols = pl.ds(pl.multiple_of(j * TILE, TILE), TILE)
            real_rows = gathered[s, :, 0, :, cols].reshape(total, TILE)
            imag_rows = gathered[s, :, 1, :, cols].reshape(total, TILE)
            for i in range(total // TILE):
                rows = onehot[i * TILE : (i + 1) * TILE, :]
                real = jnp.dot(rows, real_rows, preferred_element_type=F32)
                imag = jnp.dot(rows, imag_rows, preferred_element_type=F32)
                real_b = real.astype(BF16)
                imag_b = imag.astype(BF16)
                minus_b = (-imag).astype(BF16)
                for b in range(groups):
                    part = slice(b * depth, (b + 1) * depth)
                    at = (i * groups + b) * 2 * depth
                    wide[s - 1, 0, at : at + depth, cols] = real_b[part]
                    wide[s - 1, 0, at + depth : at + 2 * depth, cols] = minus_b[part]
                    wide[s - 1, 1, at : at + depth, cols] = imag_b[part]
                    wide[s - 1, 1, at + depth : at + 2 * depth, cols] = real_b[part]

    low_half = lax.broadcasted_iota(jnp.int32, (chunk, LANES), 1) < LANES // 2

    def pack(step, k, j, real, imag):
        for t in range(TILE // LANES):
            re = real[:, t * LANES : (t + 1) * LANES]
            im = imag[:, t * LANES : (t + 1) * LANES]
            first = jnp.where(low_half, re, pltpu.roll(im, LANES // 2, 1))
            second = jnp.where(low_half, pltpu.roll(re, LANES // 2, 1), im)
            base = (j * (TILE // LANES) + t) * 2
            send[step, k, base] = first.astype(BF16)
            send[step, k, base + 1] = second.astype(BF16)

    def swap_start(step, k):
        recv[step, k, me] = send[step, k, me]

        @pl.loop(1, n)
        def _(hop):
            target = lax.rem(me + hop, n)
            remote(
                send.at[step, k, target], recv.at[step, k, me], as_sem.at[step, k], ar_sem.at[step, k],
                {"inner": target},
            ).start()

    def swap_wait(step, k):
        part = pl.ds(0, n - 1)
        return remote(
            send.at[step, k, part], recv.at[step, k, part], as_sem.at[step, k], ar_sem.at[step, k], core_peer
        )

    def first_section(k):
        rows = slice(k * chunk, (k + 1) * chunk)

        @pl.loop(0, columns // TILE)
        def _(j):
            cols = pl.ds(pl.multiple_of(j * TILE, TILE), TILE)
            real_rows = gathered[0, :, 0, :, cols].reshape(total, TILE)
            imag_rows = gathered[0, :, 1, :, cols].reshape(total, TILE)
            a, b = picked[0, rows, :], picked[1, rows, :]
            dot = functools.partial(jnp.dot, preferred_element_type=F32)
            pack(0, k, j, dot(a, real_rows) - dot(b, imag_rows), dot(a, imag_rows) + dot(b, real_rows))

    def later_section(s, k):
        rows = slice(k * chunk, (k + 1) * chunk)

        @pl.loop(0, columns // TILE)
        def _(j):
            cols = pl.ds(pl.multiple_of(j * TILE, TILE), TILE)
            left = jnp.concatenate([recv[s - 1, k, g] for g in range(n)], axis=1)
            real = jnp.dot(left, wide[s - 1, 0, :, cols], preferred_element_type=F32)
            imag = jnp.dot(left, wide[s - 1, 1, :, cols], preferred_element_type=F32)
            if s < sections - 1:
                pack(s, k, j, real, imag)
            else:
                out[0, rows, cols] = real.astype(BF16)
                out[1, rows, cols] = imag.astype(BF16)

    def out_copy(k):
        rows = slice(k * chunk, (k + 1) * chunk)
        return pltpu.make_async_copy(out.at[:, rows], out_hbm.at[:, rows], out_sem.at[k])

    begin_z(0)
    begin_side(0)
    build_onehot(0)
    stem_copy.wait()
    pick_stem()
    for t in range(1, nz):
        z_step(0, t)
        side_send(0, t)
        if t == 1:
            begin_z(1)
        else:
            z_step(1, t - 1)
        if t == nz - 1:
            begin_z(2)
        side_step(0, t - 1)
        if t >= 2:
            diagonal_step(0, t - 2)
    side_step(0, nz - 1)
    z_step(1, nz - 1)
    diagonal_step(0, nz - 2)
    z_step(2, 1)
    diagonal_step(0, nz - 1)
    begin_side(1)
    for t in range(1, nz):
        side_send(1, t)
    finish(0)
    for k in range(CHUNKS):
        first_section(k)
        swap_start(0, k)
        if k == 0:
            for t in range(2, nz):
                z_step(2, t)
    for t in range(nz):
        side_step(1, t)
    for t in range(nz):
        diagonal_step(1, t)
    begin_side(2)
    for t in range(1, nz):
        side_send(2, t)
    finish(1)
    prepare(1)
    for k in range(CHUNKS):
        swap_wait(0, k).wait_recv()
        later_section(1, k)
        swap_start(1, k)
        if k == CHUNKS - 2:
            for t in range(nz):
                side_step(2, t)
            for t in range(nz):
                diagonal_step(2, t)
    finish(2)
    prepare(2)
    for k in range(CHUNKS):
        swap_wait(1, k).wait_recv()
        later_section(2, k)
        out_copy(k).start()

    for step in range(sections - 1):
        for k in range(CHUNKS):
            swap_wait(step, k).wait_send()
    for s in range(sections):
        for t in range(nz - 1):
            for way in (0, 1):
                @pl.when(z_sends(t, way))
                def _():
                    z_copy(s, t, way).wait_send()
        for zz in range(nz):
            @pl.when(z != zz)
            def _():
                x_copy(s, zz).wait_send()

            y_copy(s, zz).wait_send()
            diagonal_y(s, zz).wait_send()
        half = gathered.at[s, pl.ds(0, n // CORES)]
        remote(half, half, cs_sem.at[s], cr_sem.at[s], core_peer).wait_send()
    for k in range(CHUNKS):
        out_copy(k).wait()


def fused(n, stem_slab, branches, column_order):
    sections, _, depth, columns = branches.shape
    rows = stem_slab.shape[1]
    chunk = rows // CHUNKS
    nz = n // (CORES * YS)
    total = n * depth
    dma = pltpu.SemaphoreType.DMA
    return pl.pallas_call(
        functools.partial(kernel, n),
        out_shape=jax.ShapeDtypeStruct(stem_slab.shape, BF16),
        in_specs=[pl.BlockSpec(memory_space=pl.ANY)] + [pl.BlockSpec(memory_space=pltpu.VMEM)] * 2,
        out_specs=pl.BlockSpec(memory_space=pl.ANY),
        scratch_shapes=[
            pltpu.VMEM(stem_slab.shape, BF16),
            pltpu.VMEM(stem_slab.shape, BF16),
            pltpu.VMEM((sections, n, 2, depth, columns), BF16),
            pltpu.VMEM((total, total), BF16),
            pltpu.VMEM(stem_slab.shape, BF16),
            pltpu.VMEM((sections - 1, 2, 2 * total, columns), BF16),
            pltpu.VMEM((sections - 1, CHUNKS, n, chunk, LANES), BF16),
            pltpu.VMEM((sections - 1, CHUNKS, n, chunk, LANES), BF16),
            dma((sections,)),
            dma((sections, nz, 2)),
            dma((sections, nz, 2)),
            *[dma((sections, nz))] * 6,
            dma((sections,)),
            dma((sections,)),
            dma((sections - 1, CHUNKS)),
            dma((sections - 1, CHUNKS)),
            dma,
            dma((CHUNKS,)),
        ],
        compiler_params=pltpu.CompilerParams(
            collective_id=0, has_side_effects=True, vmem_limit_bytes=60 * 2**20
        ),
    )(stem_slab, branches, column_order)


def solution(mesh):
    n = mesh.shape["inner"]

    def local(stem_slab, branches, column_order):
        columns = branches.shape[3]
        fits = mesh.shape["parts"] == 2 and 2 * (columns // n) == LANES and n % (CORES * YS) == 0 and n > CORES * YS
        if fits and branches.shape[0] == 3 and columns == n * branches.shape[2]:
            return fused(n, stem_slab, branches, column_order)
        return plain(stem_slab, branches, column_order)

    in_specs = (P(None, ("parts", "inner"), None), P(None, None, "inner", None), P())
    out_specs = P(None, ("parts", "inner"), None)
    return jax.shard_map(local, mesh=mesh, in_specs=in_specs, out_specs=out_specs, check_vma=False)
```
